32 devices in a mesh: expert: 4 (over y, core), mp: 2 (over x), dp: 4 (over z).
Axes of the slice: x: 2, y: 2, z: 4, core: 2. Of those that a mesh axis runs over, the one named last changes fastest.
Arguments:
- tokens: bfloat16 [256, 4096], P(('expert', 'dp'), 'mp'), may hold values from -6 to 6
- rotation: bfloat16 [4096, 4096], P('mp', ('expert', 'dp')), may hold values from -0.09375 to 0.09375
- expert_ids: int32 [256, 2], P(('expert', 'dp')), may hold values from 0 to 3, all different within a row; in each aligned block of 16 rows (0 to 15, 16 to 31, ...) at most 12 rows name the same one
- combine: float32 [256, 2], P(('expert', 'dp')), may hold values from 0.1 to 1
- w_gate: bfloat16 [4, 14336, 4096], P('expert', ('mp', 'dp')), may hold values from -0.09375 to 0.09375
- w_up: bfloat16 [4, 14336, 4096], P('expert', ('mp', 'dp')), may hold values from -0.09375 to 0.09375
- w_down: bfloat16 [4, 14336, 4096], P('expert', ('mp', 'dp')), may hold values from -0.046875 to 0.046875
- clip_scale: float32 [4, 14336], P('expert', ('mp', 'dp')), may hold values from 0.25 to 2
- cotangent: bfloat16 [256, 4096], P(('expert', 'dp'), 'mp'), may hold values from -2 to 2
Outputs:
- layer_out: bfloat16 [256, 4096], P(('expert', 'dp'), 'mp')
- rotation_grad: float32 [4096, 4096], P('mp', ('expert', 'dp'))
The draws below stay inside these ranges and needn't reach their ends.
Inputs may be any that keep to these rules, and one draw needn't show every extreme that they name: `expert_ids`: each token names 2 different experts. In each aligned block of 16 tokens (the tokens of one index of expert and dp), no expert is named by more than 12 tokens, a bound that some block reaches.
All inputs are finite; a program needn't handle non-finite values.
Results may differ from the reference program's by a relative error of at most 0.0098.
Values may be sent and summed in bfloat16 or wider, within the bound.
A program may use at most 128 MiB of HBM per device.

```python
import math
import jax
import jax.numpy as jnp
import numpy as np
from jax import lax

D = 4096
FF = 14336
TOP = 2
HB = 64
TOK_DEV = 16
EXPERTS = 4
CAP = 12
TOKENS = 256


def block_scale(own_key, shape, split, low, largest):
    def one(position, parts):
        heights = jax.random.uniform(jax.random.fold_in(jax.random.fold_in(own_key, 6), position), (parts,), jnp.float32, low / len(split), largest / len(split))
        return jnp.repeat(jnp.exp(heights), shape[position] // parts).reshape((-1,) + (1,) * (len(shape) - position - 1))

    factor_of = one(*split[0])
    for cut in split[1:]:
        factor_of = factor_of * one(*cut)
    return factor_of


def shared_out(stream_key, own, number, rows, count, top, limit, slope):
    order = jax.random.permutation(stream_key, count)
    heavy_load, usual = portions_of(count, rows * top, limit, slope, True), portions_of(count, rows * top, limit, slope, False)
    places = jnp.arange(count)

    def named(sizes, turn):
        used = int((sizes > 0).sum())
        fixed = max(1, used // 4)
        passed = fixed + (places - fixed + turn * (used - fixed)) % max(1, count - fixed)
        return jnp.zeros((count,), jnp.int32).at[order[jnp.where(places < fixed, places, passed)]].set(jnp.asarray(sizes, jnp.int32))

    sizes = jnp.where(number % 4 == 0, named(heavy_load, number // 4), named(usual, number - number // 4 - 1))
    mixed = jax.random.permutation(jax.random.fold_in(own, 3), count)
    source_of, receiver = mixed[0:count // 2 * 2:2], mixed[1:count // 2 * 2:2]
    slack = jnp.minimum(sizes[source_of] - 1, limit - sizes[receiver]) // 2
    slack = jnp.where((source_of == order[0]) | (receiver == order[0]) | (sizes[receiver] == 0), 0, jnp.maximum(slack, 0))
    passed = jax.random.randint(jax.random.fold_in(own, 4), (count // 2,), 0, 1 << 20) % (slack + 1)
    sizes = sizes.at[source_of].add(-passed).at[receiver].add(passed)
    items = jnp.searchsorted(jnp.cumsum(sizes), jnp.arange(rows * top), side="right").astype(jnp.int32)
    table = items.reshape(top, rows).T
    table = table[jax.random.permutation(jax.random.fold_in(own, 1), rows)]
    turn = jax.random.randint(jax.random.fold_in(own, 2), (rows, 1), 0, top)
    return jnp.take_along_axis(table, (jnp.arange(top)[None, :] + turn) % top, axis=1)


def portions_of(number_of, total, reach, skew, full):
    portions = [(1 << 20) // math.isqrt(rank ** skew) + 1 for rank in range(1, number_of + 1)]
    largest = reach if full else min(reach, max(-(-total // number_of), total * portions[0] // sum(portions)))
    least = 1 if total - largest >= number_of - 1 else 0
    holding, surplus = [largest] + [least] * (number_of - 1), total - largest - least * (number_of - 1)
    while surplus > 0:
        movable = [i for i in range(1, number_of) if holding[i] < largest] or [i for i in range(1, number_of) if holding[i] < reach]
        pool, budget = sum([portions[i] for i in movable]), surplus
        for i in movable:
            extra = min(reach - holding[i], max(1, budget * portions[i] // pool), surplus)
            holding[i] = holding[i] + extra
            surplus = surplus - extra
    return np.array(holding)


def bell_draw(own_key, shape, spread, bound, cuts=(), kind=jnp.bfloat16):
    level = block_scale(own_key, shape, cuts, -0.22, 0.18) if cuts else 1.0
    entries = jax.random.normal(own_key, shape, jnp.float32) * spread * level
    return jnp.minimum(jnp.maximum(entries, -bound), bound).astype(kind)


def setup_inputs(seed: int = 0) -> dict:
    key_of = jax.random.split(jax.random.key(seed), 10)
    tokens = bell_draw(key_of[0], (TOKENS, D), 1.0, 6.0, ((0, 16), (1, 2)))
    rotation = bell_draw(key_of[1], (D, D), D ** -0.5, 0.09375, ((0, 2), (1, 16)))
    expert_ids_keys = jax.random.split(jax.random.fold_in(key_of[2], 1), TOKENS // TOK_DEV)
    expert_ids_turns = jax.random.permutation(jax.random.fold_in(key_of[2], 3), TOKENS // TOK_DEV)
    expert_ids = jax.vmap(lambda own, number: shared_out(jax.random.fold_in(key_of[2], 2), own, number, TOK_DEV, EXPERTS, TOP, CAP, 2))(expert_ids_keys, expert_ids_turns).reshape((TOKENS, TOP))
    combine = jnp.clip(0.1 + 0.9 * jax.random.uniform(key_of[3], (TOKENS, TOP), jnp.float32) ** block_scale(key_of[3], (TOKENS, TOP), ((0, 16),), -0.2, 0.2), 0.1, 1.0)
    w_gate = bell_draw(key_of[4], (EXPERTS, FF, D), D ** -0.5, 0.09375, ((0, 4), (1, 8)))
    w_up = bell_draw(key_of[5], (EXPERTS, FF, D), D ** -0.5, 0.09375, ((0, 4), (1, 8)))
    w_down = bell_draw(key_of[6], (EXPERTS, FF, D), FF ** -0.5, 0.046875, ((0, 4), (1, 8)))
    clip_scale = jnp.clip(jnp.exp(math.log(2.0) - 2.0794415 * jax.random.uniform(key_of[7], (EXPERTS, FF), jnp.float32) ** block_scale(key_of[7], (EXPERTS, FF), ((0, 4), (1, 8)), -0.2, 0.2)), 0.25, 2.0)
    cotangent = bell_draw(key_of[8], (TOKENS, D), 0.3, 2.0, ((0, 16), (1, 2)))
    return dict(tokens=tokens, rotation=rotation, expert_ids=expert_ids, combine=combine, w_gate=w_gate, w_up=w_up, w_down=w_down, clip_scale=clip_scale, cotangent=cotangent)


def hadamard_table(block_size):
    bit_index = jnp.arange(block_size, dtype=jnp.int32)
    common_bits = jnp.bitwise_and(bit_index[:, None], bit_index[None, :])
    parity = jnp.zeros((block_size, block_size), jnp.int32)
    for bit_pos in range(block_size.bit_length() - 1):
        parity = parity + jnp.bitwise_and(jnp.right_shift(common_bits, bit_pos), 1)
    sign_table = 1 - 2 * (parity % 2)
    return sign_table.astype(jnp.float32) / math.sqrt(block_size)

def blocked(values, hadamard):
    row_count, col_count = values.shape
    block_size = hadamard.shape[0]
    blocks_view = values.reshape(row_count, col_count // block_size, block_size)
    mixed = jnp.einsum('rbk,kj->rbj', blocks_view, hadamard, precision=lax.Precision.HIGHEST)
    return mixed.reshape(row_count, col_count)

def reference(tokens, rotation, expert_ids, combine, w_gate, w_up, w_down, clip_scale, cotangent):
    rotated = jnp.dot(tokens, rotation, preferred_element_type=jnp.float32).astype(jnp.bfloat16)
    total_tok, model_width = tokens.shape
    block_count = total_tok // TOK_DEV
    buffer_rows = block_count * CAP
    labels = jnp.arange(EXPERTS, dtype=jnp.int32)
    expert_hits = expert_ids[:, :, None] == labels[None, None, :]
    member = jnp.any(expert_hits, axis=1).astype(jnp.int32)
    weight = lax.optimization_barrier(jnp.sum(jnp.where(expert_hits, combine[:, :, None], 0.0), axis=1))
    per_block = member.reshape(block_count, TOK_DEV, EXPERTS)
    slot_rank = (jnp.cumsum(per_block, axis=1) - per_block).reshape(total_tok, EXPERTS)
    block_of = jnp.arange(total_tok, dtype=jnp.int32) // TOK_DEV
    slot_table = jnp.where(member > 0, block_of[:, None] * CAP + slot_rank, buffer_rows).astype(jnp.int32)
    cot_wide = cotangent.astype(jnp.float32)
    hadamard = hadamard_table(HB)

    def per_expert(running, inputs):
        out_sum, grad_sum = running
        gate_w, up_w, down_w, clip_row, slot_col, member_col, weight_col = inputs
        empty = jnp.zeros((buffer_rows + 1, model_width), jnp.bfloat16)
        expert_in = empty.at[slot_col].set(rotated)[:buffer_rows]
        cot_rows = (weight_col[:, None] * cot_wide).astype(jnp.bfloat16)
        expert_cot = empty.at[slot_col].set(cot_rows)[:buffer_rows]
        gate_act = jnp.dot(expert_in, gate_w.T, preferred_element_type=jnp.float32)
        up_act = jnp.dot(expert_in, up_w.T, preferred_element_type=jnp.float32)
        gate_sig = jax.nn.sigmoid(gate_act)
        hidden = gate_act * gate_sig * up_act
        squash = jnp.tanh(blocked(hidden, hadamard) / clip_row)
        quant = (clip_row * squash).astype(jnp.bfloat16)
        expert_out = jnp.dot(quant, down_w, preferred_element_type=jnp.float32).astype(jnp.bfloat16)
        d_quant = jnp.dot(expert_cot, down_w.T, preferred_element_type=jnp.float32)
        d_hidden = blocked(d_quant * (1.0 - squash * squash), hadamard)
        d_gate = (d_hidden * up_act * gate_sig * (1.0 + gate_act * (1.0 - gate_sig))).astype(jnp.bfloat16)
        d_up = (d_hidden * gate_act * gate_sig).astype(jnp.bfloat16)
        expert_grad = (jnp.dot(d_gate, gate_w, preferred_element_type=jnp.float32) + jnp.dot(d_up, up_w, preferred_element_type=jnp.float32)).astype(jnp.bfloat16)
        safe_slot = jnp.minimum(slot_col, buffer_rows - 1)
        live = member_col.astype(jnp.float32)
        out_sum = out_sum + (weight_col * live)[:, None] * expert_out[safe_slot].astype(jnp.float32)
        grad_sum = grad_sum + live[:, None] * expert_grad[safe_slot].astype(jnp.float32)
        return ((out_sum, grad_sum), None)
    start_sums = (jnp.zeros((total_tok, model_width), jnp.float32), jnp.zeros((total_tok, model_width), jnp.float32))
    inputs = (w_gate, w_up, w_down, clip_scale, slot_table.T, member.T, weight.T)
    (out_sum, grad_sum), unused = lax.scan(per_expert, start_sums, inputs)
    layer_out = out_sum.astype(jnp.bfloat16)
    d_rotated = grad_sum.astype(jnp.bfloat16)
    rotation_grad = jnp.dot(tokens.T, d_rotated, preferred_element_type=jnp.float32)
    return (layer_out, rotation_grad)
```

```python
import functools
import math

import jax
import jax.numpy as jnp
import numpy as np
from jax import lax
from jax.experimental import pallas as pl
from jax.experimental.pallas import tpu as pltpu
from jax.sharding import PartitionSpec as P

HB = 64


def sign_table(width):
    row = lax.broadcasted_iota(jnp.int32, (width, width), 0)
    col = lax.broadcasted_iota(jnp.int32, (width, width), 1)
    common = jnp.bitwise_and(jnp.bitwise_and(row, col), HB - 1)
    parity = jnp.zeros((width, width), jnp.int32)
    for bit_pos in range(HB.bit_length() - 1):
        parity = parity + jnp.bitwise_and(jnp.right_shift(common, bit_pos), 1)
    sign = (1 - 2 * jnp.bitwise_and(parity, 1)).astype(jnp.float32)
    same = jnp.right_shift(row, HB.bit_length() - 1) == jnp.right_shift(col, HB.bit_length() - 1)
    return jnp.where(same, sign, 0.0).astype(jnp.bfloat16)


def mix(values, table):
    high = values.astype(jnp.bfloat16)
    low = (values - high.astype(jnp.float32)).astype(jnp.bfloat16)
    total = jnp.dot(high, table, preferred_element_type=jnp.float32)
    total = total + jnp.dot(low, table, preferred_element_type=jnp.float32)
    return total * (1.0 / math.sqrt(HB))


NT = (((1,), (1,)), ((), ()))


def expert_kernel(x_ref, c_ref, w_ref, clip_ref, table_ref, gw_ref, uw_ref, dw_ref, out_ref, grad_ref):
    step = pl.program_id(0)

    @pl.when(step == 0)
    def _():
        out_ref[...] = jnp.zeros_like(out_ref)
        grad_ref[...] = jnp.zeros_like(grad_ref)

    table = table_ref[...]
    clip = clip_ref[0]
    x = x_ref[...]
    gate_act = lax.dot_general(x, gw_ref[...], NT, preferred_element_type=jnp.float32)
    up_act = lax.dot_general(x, uw_ref[...], NT, preferred_element_type=jnp.float32)
    d_quant = lax.dot_general(c_ref[...], dw_ref[...], NT, preferred_element_type=jnp.float32)
    gate_sig = jax.nn.sigmoid(gate_act)
    silu = gate_act * gate_sig
    squash = jnp.tanh(mix(silu * up_act, table) / clip)
    quant = (clip * squash).astype(jnp.bfloat16)
    d_hidden = mix(d_quant * (1.0 - squash * squash), table)
    d_gate = (d_hidden * up_act * gate_sig * (1.0 + gate_act * (1.0 - gate_sig))).astype(jnp.bfloat16)
    d_up = (d_hidden * silu).astype(jnp.bfloat16)
    weight = w_ref[...]
    width = out_ref.shape[1]
    chunk = 512 if width % 512 == 0 else width

    @pl.loop(0, width // chunk)
    def _(i):
        cols = pl.ds(pl.multiple_of(i * chunk, chunk), chunk)
        out_ref[:, cols] += weight * jnp.dot(quant, dw_ref[:, cols], preferred_element_type=jnp.float32)
        grad_ref[:, cols] += jnp.dot(d_gate, gw_ref[:, cols], preferred_element_type=jnp.float32) + jnp.dot(
            d_up, uw_ref[:, cols], preferred_element_type=jnp.float32
        )


def expert_ffn(x, c, weight, clip, gate_w, up_w, down_w):
    rows, width = x.shape
    hidden = gate_w.shape[0]
    block = max(b for b in range(HB, 257, HB) if hidden % b == 0)
    steps = hidden // block
    table = sign_table(block)
    whole = lambda shape: pl.BlockSpec(shape, lambda s: (0,) * len(shape), pipeline_mode=pl.Buffered(1))
    wspec = pl.BlockSpec((block, width), lambda s: (s, 0))
    return pl.pallas_call(
        expert_kernel,
        grid=(steps,),
        in_specs=[
            whole((rows, width)),
            whole((rows, width)),
            whole((rows, 1)),
            pl.BlockSpec((1, 1, block), lambda s: (s, 0, 0)),
            whole((block, block)),
            wspec,
            wspec,
            wspec,
        ],
        out_specs=[pl.BlockSpec((rows, width), lambda s: (0, 0), pipeline_mode=pl.Buffered(1))] * 2,
        out_shape=[jax.ShapeDtypeStruct((rows, width), jnp.float32)] * 2,
        compiler_params=pltpu.CompilerParams(vmem_limit_bytes=60 * 1024 * 1024),
        cost_estimate=pl.CostEstimate(
            flops=12 * rows * hidden * width, bytes_accessed=6 * hidden * width, transcendentals=2 * rows * hidden
        ),
    )(x, c, weight, clip.reshape(steps, 1, block), table, gate_w, up_w, down_w)


def local(tokens, rotation, expert_ids, combine, w_gate, w_up, w_down, clip_scale, cotangent):
    n_expert = lax.axis_size("expert")
    tok_axes = ("expert", "dp")
    labels = jnp.arange(n_expert, dtype=jnp.int32)
    hits = expert_ids[:, :, None] == labels[None, None, :]
    weight = jnp.sum(jnp.where(hits, combine[:, :, None], 0.0), axis=1)
    token_all = lax.all_gather(tokens, tok_axes, axis=0, tiled=True)
    part_cols = jnp.dot(token_all, rotation, preferred_element_type=jnp.float32)
    block_cols = lax.psum(part_cols, "mp").astype(jnp.bfloat16)
    rotated = lax.all_gather(block_cols, tok_axes, axis=1, tiled=True)
    weight_all = lax.all_gather(weight, tok_axes, axis=0, tiled=True)
    mine = lax.dynamic_slice_in_dim(weight_all, lax.axis_index("expert"), 1, 1)
    cot_half = lax.all_gather(cotangent, "mp", axis=1, tiled=True)
    cot_all = lax.all_gather(cot_half, tok_axes, axis=0, tiled=True)
    expert_cot = (mine * cot_all.astype(jnp.float32)).astype(jnp.bfloat16)
    out_part, grad_part = expert_ffn(
        rotated, expert_cot, mine, clip_scale[0], w_gate[0], w_up[0], w_down[0]
    )
    out_rows = lax.psum_scatter(out_part, tok_axes, scatter_dimension=0, tiled=True)
    layer_out = lax.psum_scatter(out_rows, "mp", scatter_dimension=1, tiled=True).astype(jnp.bfloat16)
    grad_cols = lax.psum_scatter(grad_part, tok_axes, scatter_dimension=1, tiled=True)
    d_rotated = lax.psum(grad_cols, "mp").astype(jnp.bfloat16)
    rotation_grad = lax.dot_general(
        token_all, d_rotated, (((0,), (0,)), ((), ())), preferred_element_type=jnp.float32
    )
    return (layer_out, rotation_grad)


def solution(mesh):
    return jax.shard_map(
        local,
        mesh=mesh,
        in_specs=(
            P(("expert", "dp"), "mp"),
            P("mp", ("expert", "dp")),
            P(("expert", "dp"), None),
            P(("expert", "dp"), None),
            P("expert", ("mp", "dp"), None),
            P("expert", ("mp", "dp"), None),
            P("expert", ("mp", "dp"), None),
            P("expert", ("mp", "dp")),
            P(("expert", "dp"), "mp"),
        ),
        out_specs=(P(("expert", "dp"), "mp"), P("mp", ("expert", "dp"))),
        check_vma=False,
    )
```
